256 devices in a mesh: nest: 4 (over y), tile: 64 (over z, x, core).
Axes of the slice: x: 4, y: 4, z: 8, core: 2. Of those that a mesh axis runs over, the one named last changes fastest.
Arguments:
- child_fields: float32 [4, 32, 1536, 3072], P('nest', None, 'tile'), may hold values from -18 to 18
- row_weights: float32 [8, 24], replicated
- col_weights: float32 [3072, 1024], replicated
- nest_offsets: int32 [4, 2], replicated, may hold values from 0 to 1023, as said below
- priority: int32 [1024, 1024], P('tile', 'nest'), may hold values from -1 to 3, as said below
- parent_old: float32 [32, 1024, 1024], P(None, 'tile', 'nest'), may hold values from -6 to 6
- smooth_rate: float32 [32], replicated, may hold values from 0.03 to 0.22
Outputs:
- parent_new: float32 [32, 1024, 1024], P(None, 'tile', 'nest')
The draws below stay inside these ranges and needn't reach their ends.
Inputs may be any that keep to these rules, and one draw needn't show every extreme that they name: nest_offsets[n, 0] lies in 0 .. 512 and nest_offsets[n, 1] in 0 .. 1023. priority[x, y] is -1 or a nest n with nest_offsets[n, 0] <= y < nest_offsets[n, 0] + 512.
All inputs are finite; a program needn't handle non-finite values.
Results may differ from the reference program's by a relative error of at most 0.000058.
Values sent between devices are 32-bit elements; how exact they have to be, the bound alone decides.
No kernel may reach another device: no remote copies, remote signals or barrier semaphores. Data moves between devices by JAX's collectives and lax.ppermute only.
A program may use at most 128 MiB of HBM per device.

```python
import math
import jax
import jax.numpy as jnp
from jax import lax

CROW = 24
FL = 32
PRD = 8
PCOLS = 1024
CW = 3072
CROWS_ALL = 1536
NR = 512
PROWS_ALL = 1024
NESTS = 4


def nest_layout(key):
    key_top, key_left, key_score, key_skip, key_order = jax.random.split(jax.random.fold_in(key, 7), 5)
    top_rows = jax.random.randint(key_top, (NESTS,), 0, PROWS_ALL - NR + 1)
    left_cols = jax.random.randint(key_left, (NESTS,), 0, PCOLS)
    order = jax.random.permutation(key_order, NESTS)
    top_rows = top_rows.at[order[0]].set(PROWS_ALL - NR)
    top_rows = top_rows.at[order[1 % NESTS]].set(0)
    left_cols = left_cols.at[order[2 % NESTS]].set(PCOLS - 1)
    left_cols = left_cols.at[order[3 % NESTS]].set(0)
    row_ids = jnp.arange(PROWS_ALL)
    covered = (row_ids[None, :] >= top_rows[:, None]) & (row_ids[None, :] < top_rows[:, None] + NR)
    scores = jax.random.randint(key_score, (NESTS, PCOLS, PROWS_ALL), 0, 1000) * NESTS + jnp.arange(NESTS)[:, None, None]
    scores = jnp.where(covered[:, None, :], scores, -1)
    chosen = jnp.argmax(scores, axis=0).astype(jnp.int32)
    any_cover = jnp.any(covered, axis=0)
    skipped = jax.random.randint(key_skip, (PCOLS, PROWS_ALL), 0, 4) == 0
    priority_map = jnp.where(any_cover[None, :] & jnp.logical_not(skipped), chosen, -1)
    offsets = jnp.stack([top_rows, left_cols], axis=1)
    return (offsets.astype(jnp.int32), priority_map.astype(jnp.int32))


def draw_nest_offsets(key, part):
    return nest_layout(key)[0]


def draw_priority(key, part):
    return nest_layout(key)[1]


def draw_row_weights(key, part):
    tap_weights = jax.random.uniform(key, (PRD, 3), jnp.float32, 0.5, 1.5)
    tap_weights = tap_weights / jnp.sum(tap_weights, axis=1, keepdims=True)
    col_ids = jnp.arange(CROW)
    parent_ids = jnp.arange(PRD)
    matrix = jnp.zeros((PRD, CROW), jnp.float32)
    for member in range(3):
        matrix = matrix + tap_weights[:, member:member + 1] * (col_ids[None, :] == 3 * parent_ids[:, None] + member).astype(jnp.float32)
    return matrix


def draw_col_weights(key, part):
    key_inner, key_outer = jax.random.split(key)
    inner = jax.random.uniform(key_inner, (PCOLS, 3), jnp.float32, 0.5, 1.5)
    outer = jax.random.uniform(key_outer, (PCOLS, 2), jnp.float32, 0.1, 0.5)
    tap_weights = jnp.concatenate([outer[:, :1], inner, outer[:, 1:]], axis=1)
    tap_weights = tap_weights / jnp.sum(tap_weights, axis=1, keepdims=True)
    child_ids = jnp.arange(CW)
    parent_ids = jnp.arange(PCOLS)
    matrix = jnp.zeros((CW, PCOLS), jnp.float32)
    for member in range(5):
        target = (3 * parent_ids + member - 1) % CW
        matrix = matrix + tap_weights[None, :, member] * (child_ids[:, None] == target[None, :]).astype(jnp.float32)
    return matrix


def block_levels(key, extent, pieces, smallest, largest):
    loudness, own = 1.0, jax.random.fold_in(key, 6)
    for dim, shards_of in pieces:
        heights = jnp.exp(jax.random.uniform(jax.random.fold_in(own, dim), (shards_of,), jnp.float32, smallest / len(pieces), largest / len(pieces)))
        loudness = loudness * jnp.repeat(heights, extent[dim] // shards_of).reshape([-1 if axis == dim else 1 for axis in range(len(extent))])
    return loudness


def normal_values(key, dims, deviation, limit, cuts=(), kind=jnp.bfloat16):
    gain = block_levels(key, dims, cuts, -0.22, 0.18) if cuts else 1.0
    entries = jax.random.normal(key, dims, jnp.float32) * deviation * gain
    return jnp.minimum(jnp.maximum(entries, -limit), limit).astype(kind)


def setup_inputs(seed: int = 0) -> dict:
    key_list = jax.random.split(jax.random.key(seed), 8)
    child_fields = normal_values(key_list[0], (NESTS, FL, CROWS_ALL, CW), 3.0, 18.0, ((0, 4), (2, 64)), jnp.float32)
    row_weights = draw_row_weights(jax.random.fold_in(key_list[7], 71), 0)
    col_weights = draw_col_weights(jax.random.fold_in(key_list[7], 71), 0)
    nest_offsets = draw_nest_offsets(jax.random.fold_in(key_list[7], 71), 0)
    priority = draw_priority(jax.random.fold_in(key_list[7], 71), 0)
    parent_old = normal_values(key_list[5], (FL, PCOLS, PROWS_ALL), 1.0, 6.0, ((1, 64), (2, 4)), jnp.float32)
    smooth_rate = jnp.clip(jnp.exp(jax.random.uniform(key_list[6], (FL,), jnp.float32, math.log(0.03), math.log(0.22))), 0.03, 0.22)
    return {"child_fields": child_fields, "row_weights": row_weights, "col_weights": col_weights, "nest_offsets": nest_offsets, "priority": priority, "parent_old": parent_old, "smooth_rate": smooth_rate}


def reference(child_fields, row_weights, col_weights, nest_offsets, priority, parent_old, smooth_rate):
    nest_count, planes, crows_all, child_cols = child_fields.shape
    cell_rows, child_rows = row_weights.shape
    row_blocks = crows_all // child_rows
    nrows = row_blocks * cell_rows

    def restrict_one(child_block):
        grouped = child_block.reshape(planes, row_blocks, child_rows, child_cols)
        thinned = jnp.einsum('pr,ftrc->ftpc', row_weights, grouped, precision=lax.Precision.HIGHEST)
        thinned = thinned.reshape(planes, nrows, child_cols)
        return jnp.einsum('fyc,cx->fxy', thinned, col_weights, precision=lax.Precision.HIGHEST)

    restricted = lax.map(restrict_one, child_fields)
    merged = parent_old
    for nest_num in range(nest_count):
        rolled = jnp.roll(restricted[nest_num], nest_offsets[nest_num, 1], axis=1)
        placed = lax.dynamic_update_slice(jnp.zeros_like(parent_old), rolled,
                                          (jnp.int32(0), jnp.int32(0), nest_offsets[nest_num, 0].astype(jnp.int32)))
        merged = jnp.where((priority == nest_num)[None], placed, merged)
    east_side = jnp.roll(merged, -1, axis=1)
    west_side = jnp.roll(merged, 1, axis=1)
    padded = jnp.concatenate([merged[:, :, :1], merged, merged[:, :, -1:]], axis=2)
    north_side = padded[:, :, 2:]
    south_side = padded[:, :, :-2]
    return merged + smooth_rate[:, None, None] * (east_side + west_side + north_side + south_side - 4.0 * merged)
```

```python
import functools

import jax
import jax.numpy as jnp
from jax import lax
from jax.experimental import pallas as pl
from jax.experimental.pallas import tpu as pltpu
from jax.sharding import PartitionSpec as P


LANES = 128
STRIP = 16
GROUP = 8
CELLS = 8
ROWS = 9


def pack_kernel(shift_ref, r_ref, out_ref, turned, columns):
    shift = shift_ref[0]
    whole, part = shift // LANES, shift % LANES
    blocks = r_ref.shape[1] // LANES
    width = r_ref.shape[0]
    strips = LANES // STRIP
    tiles = blocks * strips
    lane = lax.broadcasted_iota(jnp.int32, (width, LANES), 1)
    for k in range(blocks):
        turned[k] = pltpu.roll(r_ref[:, k * LANES : (k + 1) * LANES], part, 1)
    for k in range(blocks):
        here = turned[lax.rem(k + blocks - whole, blocks)]
        before = turned[lax.rem(k + 2 * blocks - 1 - whole, blocks)]
        block = jnp.where(lane >= part, here, before).T
        for jj in range(width // LANES):
            row = jj * r_ref.shape[1] + k * LANES
            columns[row : row + LANES, :] = block[:, jj * LANES : (jj + 1) * LANES]
    low = lax.broadcasted_iota(jnp.int32, (8, LANES), 1) < LANES // 2
    low_all = lax.broadcasted_iota(jnp.int32, (tiles, LANES), 1) < LANES // 2
    half = LANES // 2
    for jj in range(width // LANES):
        base = jj * r_ref.shape[1]
        for t in range(tiles):
            row = base + t * STRIP
            first, second = columns[row : row + 8, :], columns[row + 8 : row + 16, :]
            row = (2 * jj * tiles + t) * ROWS
            out_ref[row : row + 8, :] = jnp.where(low, first, pltpu.roll(second, half, 1))
            row = ((2 * jj + 1) * tiles + t) * ROWS
            out_ref[row : row + 8, :] = jnp.where(low, pltpu.roll(first, half, 1), second)
        west = pltpu.roll(columns[pl.ds(base + STRIP - 1, tiles, stride=STRIP), :], 1, 0)
        east = pltpu.roll(columns[pl.ds(base, tiles, stride=STRIP), :], tiles - 1, 0)
        edge = jnp.where(low_all, west, pltpu.roll(east, half, 1))
        out_ref[pl.ds(2 * jj * tiles * ROWS + 8, tiles, stride=ROWS), :] = edge
        edge = jnp.where(low_all, pltpu.roll(west, half, 1), east)
        out_ref[pl.ds((2 * jj + 1) * tiles * ROWS + 8, tiles, stride=ROWS), :] = edge


def pack(restricted, shift, tiles):
    width, columns = restricted.shape
    rows = (width // (GROUP * CELLS)) * tiles * ROWS
    return pl.pallas_call(
        pack_kernel,
        out_shape=jax.ShapeDtypeStruct((rows, LANES), jnp.float32),
        in_specs=[
            pl.BlockSpec(memory_space=pltpu.SMEM),
            pl.BlockSpec(memory_space=pltpu.VMEM),
        ],
        out_specs=pl.BlockSpec(memory_space=pltpu.VMEM),
        scratch_shapes=[
            pltpu.VMEM((columns // LANES, width, LANES), jnp.float32),
            pltpu.VMEM((width // LANES * columns, LANES), jnp.float32),
        ],
        compiler_params=pltpu.CompilerParams(vmem_limit_bytes=12 * 2**20),
        name="pack",
    )(shift, restricted)


def granule_transpose(parts, granule):
    count = len(parts)
    lane = lax.broadcasted_iota(jnp.int32, parts[0].shape, parts[0].ndim - 1)
    axis = parts[0].ndim - 1
    bit = 1
    while bit < count:
        move = bit * granule
        upper = (lane & move) != 0
        done = list(parts)
        for i in range(count):
            if not i & bit:
                a, b = parts[i], parts[i | bit]
                done[i] = jnp.where(upper, pltpu.roll(b, move, axis), a)
                done[i | bit] = jnp.where(upper, b, pltpu.roll(a, LANES - move, axis))
        parts = done
        bit *= 2
    return parts


def merge_kernel(
    offset_ref, got_ref, old_ref, west_ref, east_ref, rate_ref, out_ref,
    turned, cells, chosen, edges, edge_cells, edge_chosen, edge_turned,
):
    nests = offset_ref.shape[0]
    tiles = got_ref.shape[0] // (nests * ROWS)
    span = LANES // CELLS
    groups = tiles // span
    quarters = old_ref.shape[0]
    blocks = 2 * quarters
    for b in range(blocks):
        q, at = b // 2, slice((b % 2) * LANES, (b % 2 + 1) * LANES)
        cells[b] = old_ref[q, :GROUP, :, at]
        chosen[b] = old_ref[q, GROUP, :, at]
        edge_cells[b, :GROUP] = west_ref[q, :GROUP, at]
        edge_cells[b, GROUP:] = east_ref[q, :GROUP, at]
        edge_chosen[b, :GROUP] = jnp.broadcast_to(west_ref[q, GROUP : GROUP + 1, at], (GROUP, LANES))
        edge_chosen[b, GROUP:] = jnp.broadcast_to(east_ref[q, GROUP : GROUP + 1, at], (GROUP, LANES))
    chosen[blocks] = jnp.full((STRIP, LANES), -1.0, jnp.float32)
    edge_chosen[blocks] = jnp.full((2 * GROUP, LANES), -1.0, jnp.float32)
    combos = nests * groups
    parts = granule_transpose(
        [got_ref[pl.ds(i * ROWS + 8, combos, stride=span * ROWS), :] for i in range(span)], CELLS
    )
    for k in range(span):
        edges[k * combos : (k + 1) * combos, :] = parts[k]
    lane = lax.broadcasted_iota(jnp.int32, (STRIP, LANES), 1)
    for n in range(nests):
        start = offset_ref[n, 0]
        whole, part = start // LANES, start % LANES
        for g in range(groups):
            base = (n * tiles + g * span) * ROWS
            parts = granule_transpose(
                [got_ref[base + i * ROWS : base + i * ROWS + 8, :] for i in range(span)], CELLS
            )
            for k in range(span):
                h, f = k // GROUP, k % GROUP
                turned[g + 1, f, h * 8 : h * 8 + 8] = pltpu.roll(parts[k], part, 1)
            edge_turned[g + 1] = pltpu.roll(
                edges[pl.ds(n * groups + g, span, stride=combos), :], part, 1
            )
        keep = lane >= part
        for k in range(groups + 1):
            b = whole + k
            mine = chosen[b] == n
            for f in range(GROUP):
                value = jnp.where(keep, turned[k + 1, f], turned[k, f])
                cells[b, f] = jnp.where(mine, value, cells[b, f])
            value = jnp.where(keep, edge_turned[k + 1], edge_turned[k])
            edge_cells[b] = jnp.where(edge_chosen[b] == n, value, edge_cells[b])
    row = lax.broadcasted_iota(jnp.int32, (STRIP, LANES), 0)
    for f in range(GROUP):
        rate = rate_ref[f : f + 1, :]
        mids = [cells[b, f] for b in range(blocks)]
        ups = [pltpu.roll(m, LANES - 1, 1) for m in mids]
        downs = [pltpu.roll(m, 1, 1) for m in mids]
        for b in range(blocks):
            mid = mids[b]
            north = jnp.where(lane == LANES - 1, ups[b + 1] if b + 1 < blocks else mid, ups[b])
            south = jnp.where(lane == 0, downs[b - 1] if b else mid, downs[b])
            west = jnp.where(row == 0, edge_cells[b, f : f + 1], pltpu.roll(mid, 1, 0))
            east = jnp.where(
                row == STRIP - 1, edge_cells[b, GROUP + f : GROUP + f + 1],
                pltpu.roll(mid, STRIP - 1, 0),
            )
            value = mid + rate * (east + west + north + south - 4.0 * mid)
            out_ref[b // 2, f, :, (b % 2) * LANES : (b % 2 + 1) * LANES] = value


def merge(offsets, got, old, west, east, rate):
    quarters = old.shape[0]
    blocks = 2 * quarters
    nests = offsets.shape[0]
    tiles = got.shape[0] // (nests * ROWS)
    span = LANES // CELLS
    groups = tiles // span
    vmem = pl.BlockSpec(memory_space=pltpu.VMEM)
    return pl.pallas_call(
        merge_kernel,
        out_shape=jax.ShapeDtypeStruct((quarters, GROUP, STRIP, 2 * LANES), jnp.float32),
        in_specs=[pl.BlockSpec(memory_space=pltpu.SMEM)] + [vmem] * 5,
        out_specs=vmem,
        scratch_shapes=[
            pltpu.VMEM((groups + 2, GROUP, STRIP, LANES), jnp.float32),
            pltpu.VMEM((blocks + 1, GROUP, STRIP, LANES), jnp.float32),
            pltpu.VMEM((blocks + 1, STRIP, LANES), jnp.float32),
            pltpu.VMEM((span * nests * groups, LANES), jnp.float32),
            pltpu.VMEM((blocks + 1, 2 * GROUP, LANES), jnp.float32),
            pltpu.VMEM((blocks + 1, 2 * GROUP, LANES), jnp.float32),
            pltpu.VMEM((groups + 2, 2 * GROUP, LANES), jnp.float32),
        ],
        compiler_params=pltpu.CompilerParams(vmem_limit_bytes=12 * 2**20),
        name="merge",
    )(offsets, got, old, west, east, rate)


def turn(count, by):
    return [(i, (i + by) % count) for i in range(count)]


def per_device(
    child_fields, row_weights, col_weights, nest_offsets, priority, parent_old, smooth_rate
):
    child_block = child_fields[0]
    tiles, nests = lax.axis_size("tile"), lax.axis_size("nest")
    nest_id = lax.axis_index("nest")
    thinned = jnp.einsum("pr,frc->fpc", row_weights, child_block, precision=lax.Precision.HIGHEST)
    restricted = jnp.einsum("fpc,cx->fpx", thinned, col_weights, precision=lax.Precision.HIGH)
    restricted = restricted.reshape(-1, restricted.shape[-1])
    shift = lax.dynamic_index_in_dim(nest_offsets[:, 1], nest_id, 0)
    outgoing = pack(restricted, shift, tiles)

    outgoing, parent_old, levels = lax.optimization_barrier(
        (outgoing, parent_old, priority.astype(jnp.float32))
    )
    got = lax.all_to_all(
        outgoing.reshape(nests * tiles, ROWS, 1, LANES), ("nest", "tile"),
        split_axis=0, concat_axis=0, tiled=True,
    ).reshape(nests * tiles * ROWS, LANES)

    def share(by):
        block = lax.dynamic_slice_in_dim(
            parent_old, GROUP * lax.rem(nest_id + by, nests), GROUP, axis=0
        )
        block = jnp.concatenate([block, levels[None]], axis=0)
        return lax.ppermute(block, "nest", turn(nests, by)) if by else block

    shares = [share(nests - 1 - i) for i in range(nests)]
    old = lax.dynamic_slice_in_dim(
        jnp.stack(shares + shares[:-1]), nests - 1 - nest_id, nests, axis=0
    )
    west = lax.ppermute(old[:, :, -1], "tile", turn(tiles, 1))
    east = lax.ppermute(old[:, :, 0], "tile", turn(tiles, -1))
    rate = lax.dynamic_slice_in_dim(smooth_rate, GROUP * nest_id, GROUP)
    rate = jnp.broadcast_to(rate[:, None], (GROUP, LANES))

    smoothed = merge(nest_offsets, got, old, west, east, rate)
    placed = lax.all_to_all(smoothed, "nest", split_axis=0, concat_axis=0, tiled=True)
    return placed.reshape(nests * GROUP, STRIP, 2 * LANES)


def solution(mesh):
    return jax.shard_map(
        per_device,
        mesh=mesh,
        in_specs=(
            P("nest", None, "tile", None),
            P(),
            P(),
            P(),
            P("tile", "nest"),
            P(None, "tile", "nest"),
            P(),
        ),
        out_specs=P(None, "tile", "nest"),
        check_vma=False,
    )
```

```python
import jax
import jax.numpy as jnp
from jax import lax
from jax.experimental import pallas as pl
from jax.experimental.pallas import tpu as pltpu
from jax.sharding import PartitionSpec as P


LANES = 128
STRIP = 16
GROUP = 8
CELLS = 8
ROWS = 9


def granule_transpose(parts, granule):
    count = len(parts)
    lane = lax.broadcasted_iota(jnp.int32, parts[0].shape, parts[0].ndim - 1)
    axis = parts[0].ndim - 1
    bit = 1
    while bit < count:
        move = bit * granule
        upper = (lane & move) != 0
        done = list(parts)
        for i in range(count):
            if not i & bit:
                a, b = parts[i], parts[i | bit]
                done[i] = jnp.where(upper, pltpu.roll(b, move, axis), a)
                done[i | bit] = jnp.where(upper, b, pltpu.roll(a, LANES - move, axis))
        parts = done
        bit *= 2
    return parts


def split_halves(value):
    high = value.astype(jnp.bfloat16)
    low = (value - high.astype(jnp.float32)).astype(jnp.bfloat16)
    return high, low


def restrict_kernel(
    offset_ref, row_ref, child_ref, col_ref, out_ref, taps, left, right, total, turned, columns
):
    step = pl.program_id(0)
    fields, child_rows, chunk = child_ref.shape
    cells = row_ref.shape[0]
    width = fields * cells
    all_columns = col_ref.shape[1]
    reach = GROUP * child_rows

    @pl.when(step == 0)
    def _():
        taps[...] = jnp.zeros_like(taps)
        taps[:cells, :child_rows] = row_ref[...]
        first = taps[:cells, :]
        for f in range(1, GROUP):
            taps[f * cells : (f + 1) * cells, :] = pltpu.roll(first, f * child_rows, 1)
        total[...] = jnp.zeros_like(total)

    taps_high, taps_low = split_halves(taps[:, :reach])
    taps_both = jnp.concatenate([taps_high, taps_low], axis=0)
    rows = GROUP * cells
    for g in range(fields // GROUP):
        block = child_ref[g * GROUP : (g + 1) * GROUP].reshape(reach, chunk)
        high, low = split_halves(block)
        both = jnp.dot(taps_both, high, preferred_element_type=jnp.float32)
        rest = jnp.dot(taps_high, low, preferred_element_type=jnp.float32)
        thin_high, thin_low = split_halves(both[:rows] + (both[rows:] + rest))
        at = slice(g * rows, (g + 1) * rows)
        left[at, :chunk] = thin_high
        left[at, chunk : 2 * chunk] = thin_low
        left[at, 2 * chunk :] = thin_high
    high, low = split_halves(col_ref[...])
    right[:chunk] = high
    right[chunk : 2 * chunk] = high
    right[2 * chunk :] = low
    total[...] += jnp.dot(left[...], right[...], preferred_element_type=jnp.float32)

    @pl.when(step == pl.num_programs(0) - 1)
    def _():
        shift = offset_ref[1, lax.axis_index("nest")]
        whole, part = shift // LANES, shift % LANES
        blocks = all_columns // LANES
        tiles = all_columns // STRIP
        strips = LANES // STRIP
        lane = lax.broadcasted_iota(jnp.int32, (width, LANES), 1)
        for k in range(blocks):
            turned[k] = pltpu.roll(total[:, k * LANES : (k + 1) * LANES], part, 1)

        def pack_block(i, carry):
            for k in (2 * i, 2 * i + 1):
                here = turned[lax.rem(k + blocks - whole, blocks)]
                before = turned[lax.rem(k + 2 * blocks - 1 - whole, blocks)]
                block = jnp.where(lane >= part, here, before)
                for j in range(fields // GROUP):
                    top = j * rows
                    parts = granule_transpose(
                        [block[top + f * cells : top + (f + 1) * cells] for f in range(GROUP)], STRIP
                    )
                    base = pl.multiple_of((j * tiles + k * strips) * ROWS, 8)
                    target = out_ref.at[pl.ds(base, strips * ROWS), :]
                    for t in range(strips):
                        target[t * ROWS : t * ROWS + 8, :] = parts[t]
                upright = block.T
                for jj in range(width // LANES):
                    row = pl.multiple_of(jj * all_columns + k * LANES, LANES)
                    columns[pl.ds(row, LANES), :] = upright[:, jj * LANES : (jj + 1) * LANES]
            return carry

        lax.fori_loop(0, blocks // 2, pack_block, 0)
        low_all = lax.broadcasted_iota(jnp.int32, (tiles, LANES), 1) < LANES // 2
        half = LANES // 2
        for jj in range(width // LANES):
            base = jj * all_columns
            west = pltpu.roll(columns[pl.ds(base + STRIP - 1, tiles, stride=STRIP), :], 1, 0)
            east = pltpu.roll(columns[pl.ds(base, tiles, stride=STRIP), :], tiles - 1, 0)
            edge = jnp.where(low_all, west, pltpu.roll(east, half, 1))
            out_ref[pl.ds(2 * jj * tiles * ROWS + 8, tiles, stride=ROWS), :] = edge
            edge = jnp.where(low_all, pltpu.roll(west, half, 1), east)
            out_ref[pl.ds((2 * jj + 1) * tiles * ROWS + 8, tiles, stride=ROWS), :] = edge


CHUNK = 768


def restrict(nest_offsets, row_weights, child_block, col_weights, tiles):
    fields, child_rows, child_columns = child_block.shape
    columns = col_weights.shape[1]
    cells = row_weights.shape[0]
    width = fields * cells
    rows = (fields // GROUP) * tiles * ROWS
    return pl.pallas_call(
        restrict_kernel,
        grid=(child_columns // CHUNK,),
        out_shape=jax.ShapeDtypeStruct((rows, LANES), jnp.float32),
        in_specs=[
            pl.BlockSpec(memory_space=pltpu.SMEM),
            pl.BlockSpec(row_weights.shape, lambda i: (0, 0)),
            pl.BlockSpec((fields, child_rows, CHUNK), lambda i: (0, 0, i)),
            pl.BlockSpec((CHUNK, columns), lambda i: (i, 0)),
        ],
        out_specs=pl.BlockSpec((rows, LANES), lambda i: (0, 0)),
        scratch_shapes=[
            pltpu.VMEM((GROUP * cells, 2 * LANES), jnp.float32),
            pltpu.VMEM((width, 3 * CHUNK), jnp.bfloat16),
            pltpu.VMEM((3 * CHUNK, columns), jnp.bfloat16),
            pltpu.VMEM((width, columns), jnp.float32),
            pltpu.VMEM((columns // LANES, width, LANES), jnp.float32),
            pltpu.VMEM((width // LANES * columns, LANES), jnp.float32),
        ],
        compiler_params=pltpu.CompilerParams(vmem_limit_bytes=60 * 2**20),
        cost_estimate=pl.CostEstimate(
            flops=6 * width * child_columns * columns,
            bytes_accessed=4 * (child_block.size + col_weights.size),
            transcendentals=0,
        ),
        name="restrict",
    )(nest_offsets.T, row_weights, child_block, col_weights)


def rim_kernel(old_ref, level_ref, last_ref, first_ref):
    fields = old_ref.shape[0]
    for f in range(fields):
        last_ref[f : f + 1] = old_ref[f, STRIP - 1 :]
        first_ref[f : f + 1] = old_ref[f, :1]
    level = level_ref[...].astype(jnp.float32)
    last_ref[fields:] = jnp.broadcast_to(level[STRIP - 1 :], (GROUP, 2 * LANES))
    first_ref[fields:] = jnp.broadcast_to(level[:1], (GROUP, 2 * LANES))


def rim(parent_old, priority):
    vmem = pl.BlockSpec(memory_space=pltpu.VMEM)
    shape = jax.ShapeDtypeStruct((parent_old.shape[0] + GROUP, 2 * LANES), jnp.float32)
    return pl.pallas_call(
        rim_kernel,
        out_shape=[shape] * 2,
        in_specs=[vmem] * 2,
        out_specs=[vmem] * 2,
        compiler_params=pltpu.CompilerParams(vmem_limit_bytes=4 * 2**20),
        name="rim",
    )(parent_old, priority)


SHARE = (GROUP + 1) * STRIP


def share_kernel(old_ref, level_ref, west_ref, east_ref, *outs):
    me = lax.axis_index("nest")
    nests = len(outs)
    for d in range(nests):
        first = GROUP * lax.rem(me + d, nests)
        for f in range(GROUP):
            outs[d][f * STRIP : (f + 1) * STRIP] = old_ref[first + f]
        outs[d][GROUP * STRIP : SHARE] = level_ref[...].astype(jnp.float32)
        for i, ref in enumerate((west_ref, east_ref)):
            row = SHARE + 2 * i * GROUP
            outs[d][row : row + GROUP] = ref[pl.ds(pl.multiple_of(first, GROUP), GROUP)]
            outs[d][row + GROUP : row + 2 * GROUP] = ref[nests * GROUP :]


def share(parent_old, priority, west, east):
    nests = parent_old.shape[0] // GROUP
    vmem = pl.BlockSpec(memory_space=pltpu.VMEM)
    shape = jax.ShapeDtypeStruct((SHARE + 4 * GROUP, 2 * LANES), jnp.float32)
    return pl.pallas_call(
        share_kernel,
        out_shape=[shape] * nests,
        in_specs=[vmem] * 4,
        out_specs=[vmem] * nests,
        compiler_params=pltpu.CompilerParams(vmem_limit_bytes=8 * 2**20),
        name="share",
    )(parent_old, priority, west, east)


def merge_kernel(offset_ref, got_ref, rate_ref, *refs):
    nests = offset_ref.shape[1]
    shares, out_ref = refs[:nests], refs[nests]
    slab, cells, chosen, edges, edge_cells, edge_chosen, edge_turned = refs[nests + 1 :]
    tiles = got_ref.shape[0] // (nests * ROWS)
    span = LANES // CELLS
    groups = tiles // span
    blocks = 2 * nests
    combos = nests * groups
    me = lax.axis_index("nest")
    for d in range(nests):
        q = lax.rem(me + nests - d, nests)
        ref = shares[d]
        for side in range(2):
            b, at = 2 * q + side, slice(side * LANES, (side + 1) * LANES)
            for f in range(GROUP):
                cells[b, f] = ref[f * STRIP : (f + 1) * STRIP, at]
            chosen[b] = ref[GROUP * STRIP : SHARE, at]
            for i in range(2):
                row = SHARE + 2 * i * GROUP
                rows = slice(i * GROUP, (i + 1) * GROUP)
                edge_cells[b, rows] = ref[row : row + GROUP, at]
                edge_chosen[b, rows] = ref[row + GROUP : row + 2 * GROUP, at]
    chosen[blocks] = jnp.full((STRIP, LANES), -1.0, jnp.float32)
    edge_chosen[blocks] = jnp.full((2 * GROUP, LANES), -1.0, jnp.float32)
    parts = granule_transpose(
        [got_ref[pl.ds(i * ROWS + 8, combos, stride=span * ROWS), :] for i in range(span)], CELLS
    )
    for k in range(span):
        edges[k * combos : (k + 1) * combos, :] = parts[k]
    lane = lax.broadcasted_iota(jnp.int32, (STRIP, LANES), 1)

    def place(n, carry):
        start = offset_ref[0, n]
        whole, part = start // LANES, start % LANES
        source = got_ref.at[pl.ds(pl.multiple_of(n * tiles * ROWS, 8), tiles * ROWS), :]
        for t in range(tiles):
            slab[pl.ds(part + t * CELLS, CELLS), :] = source[t * ROWS : t * ROWS + 8, :]
        for g in range(groups):
            edge_turned[g + 1] = pltpu.roll(
                edges[pl.ds(n * groups + g, span, stride=combos), :], part, 1
            )
        keep = lane >= part
        number = n.astype(jnp.float32)
        for k in range(groups + 1):
            b = whole + k
            mine = chosen[b] == number
            upright = slab[k * LANES : (k + 1) * LANES, :].T
            for f in range(GROUP):
                value = upright[f * STRIP : (f + 1) * STRIP]
                cells[b, f] = jnp.where(mine, value, cells[b, f])
            value = jnp.where(keep, edge_turned[k + 1], edge_turned[k])
            edge_cells[b] = jnp.where(edge_chosen[b] == number, value, edge_cells[b])
        return carry

    lax.fori_loop(0, nests, place, 0)
    row = lax.broadcasted_iota(jnp.int32, (STRIP, LANES), 0)

    def smooth(f, carry):
        rate = rate_ref[pl.ds(f, 1), :]
        mids = [cells[b, f] for b in range(blocks)]
        ups = [pltpu.roll(m, LANES - 1, 1) for m in mids]
        downs = [pltpu.roll(m, 1, 1) for m in mids]
        for b in range(blocks):
            mid = mids[b]
            north = jnp.where(lane == LANES - 1, ups[b + 1] if b + 1 < blocks else mid, ups[b])
            south = jnp.where(lane == 0, downs[b - 1] if b else mid, downs[b])
            west = jnp.where(row == 0, edge_cells[b, pl.ds(f, 1)], pltpu.roll(mid, 1, 0))
            east = jnp.where(
                row == STRIP - 1, edge_cells[b, pl.ds(GROUP + f, 1)],
                pltpu.roll(mid, STRIP - 1, 0),
            )
            value = mid + rate * (east + west + north + south - 4.0 * mid)
            out_ref[b // 2, f, :, (b % 2) * LANES : (b % 2 + 1) * LANES] = value
        return carry

    lax.fori_loop(0, GROUP, smooth, 0)


def merge(offsets, got, rate, shares):
    nests = len(shares)
    blocks = 2 * nests
    tiles = got.shape[0] // (nests * ROWS)
    span = LANES // CELLS
    groups = tiles // span
    vmem = pl.BlockSpec(memory_space=pltpu.VMEM)
    return pl.pallas_call(
        merge_kernel,
        out_shape=jax.ShapeDtypeStruct((nests, GROUP, STRIP, 2 * LANES), jnp.float32),
        in_specs=[pl.BlockSpec(memory_space=pltpu.SMEM)] + [vmem] * (2 + len(shares)),
        out_specs=vmem,
        scratch_shapes=[
            pltpu.VMEM(((groups + 1) * LANES, LANES), jnp.float32),
            pltpu.VMEM((blocks + 1, GROUP, STRIP, LANES), jnp.float32),
            pltpu.VMEM((blocks + 1, STRIP, LANES), jnp.float32),
            pltpu.VMEM((span * nests * groups, LANES), jnp.float32),
            pltpu.VMEM((blocks + 1, 2 * GROUP, LANES), jnp.float32),
            pltpu.VMEM((blocks + 1, 2 * GROUP, LANES), jnp.float32),
            pltpu.VMEM((groups + 2, 2 * GROUP, LANES), jnp.float32),
        ],
        compiler_params=pltpu.CompilerParams(vmem_limit_bytes=12 * 2**20),
        name="merge",
    )(offsets.T, got, rate, *shares)


def per_device(
    child_fields, row_weights, col_weights, nest_offsets, priority, parent_old, smooth_rate
):
    tiles, nests = lax.axis_size("tile"), lax.axis_size("nest")
    nest_id = lax.axis_index("nest")
    last, first = rim(parent_old, priority)
    west = lax.ppermute(last, "tile", [(t, (t + 1) % tiles) for t in range(tiles)])
    east = lax.ppermute(first, "tile", [(t, (t - 1) % tiles) for t in range(tiles)])
    outgoing = restrict(nest_offsets, row_weights, child_fields[0], col_weights, tiles)
    outgoing, west, east, parent_old, priority, smooth_rate = lax.optimization_barrier(
        (outgoing, west, east, parent_old, priority, smooth_rate)
    )
    got = lax.all_to_all(
        outgoing.reshape(nests * tiles, ROWS, 1, LANES), ("nest", "tile"),
        split_axis=0, concat_axis=0, tiled=True,
    ).reshape(nests * tiles * ROWS, LANES)

    shares = share(parent_old, priority, west, east)
    shares = [
        lax.ppermute(block, "nest", [(n, (n + d) % nests) for n in range(nests)]) if d else block
        for d, block in enumerate(shares)
    ]
    rate = lax.dynamic_slice_in_dim(smooth_rate, GROUP * nest_id, GROUP)
    rate = jnp.broadcast_to(rate[:, None], (GROUP, LANES))

    smoothed = merge(nest_offsets, got, rate, shares)
    placed = lax.all_to_all(smoothed, "nest", split_axis=0, concat_axis=0, tiled=True)
    return placed.reshape(nests * GROUP, STRIP, 2 * LANES)


def solution(mesh):
    return jax.shard_map(
        per_device,
        mesh=mesh,
        in_specs=(
            P("nest", None, "tile", None),
            P(),
            P(),
            P(),
            P("tile", "nest"),
            P(None, "tile", "nest"),
            P(),
        ),
        out_specs=P(None, "tile", "nest"),
        check_vma=False,
    )
```

```python
import jax
import jax.numpy as jnp
from jax import lax
from jax.experimental import pallas as pl
from jax.experimental.pallas import tpu as pltpu
from jax.sharding import PartitionSpec as P


LANES = 128
STRIP = 16
GROUP = 8
CELLS = 8


def granule_transpose(parts, granule):
    count = len(parts)
    lane = lax.broadcasted_iota(jnp.int32, parts[0].shape, parts[0].ndim - 1)
    axis = parts[0].ndim - 1
    bit = 1
    while bit < count:
        move = bit * granule
        upper = (lane & move) != 0
        done = list(parts)
        for i in range(count):
            if not i & bit:
                a, b = parts[i], parts[i | bit]
                done[i] = jnp.where(upper, pltpu.roll(b, move, axis), a)
                done[i | bit] = jnp.where(upper, b, pltpu.roll(a, LANES - move, axis))
        parts = done
        bit *= 2
    return parts


def split_halves(value):
    high = value.astype(jnp.bfloat16)
    low = (value - high.astype(jnp.float32)).astype(jnp.bfloat16)
    return high, low


def restrict_kernel(
    offset_ref, row_ref, child_ref, col_ref, out_ref, taps, left, total, turned
):
    step = pl.program_id(0)
    fields, child_rows, chunk = child_ref.shape
    cells = row_ref.shape[0]
    width = fields * cells
    all_columns = col_ref.shape[1]
    reach = GROUP * child_rows

    @pl.when(step == 0)
    def _():
        taps[...] = jnp.zeros_like(taps)
        taps[:cells, :child_rows] = row_ref[...]
        first = taps[:cells, :]
        for f in range(1, GROUP):
            taps[f * cells : (f + 1) * cells, :] = pltpu.roll(first, f * child_rows, 1)
        total[...] = jnp.zeros_like(total)

    taps_high, taps_low = split_halves(taps[:, :reach])
    taps_both = jnp.concatenate([taps_high, taps_low], axis=0)
    rows = GROUP * cells
    for g in range(fields // GROUP):
        block = child_ref[g * GROUP : (g + 1) * GROUP].reshape(reach, chunk)
        high, low = split_halves(block)
        both = jnp.dot(taps_both, high, preferred_element_type=jnp.float32)
        rest = jnp.dot(taps_high, low, preferred_element_type=jnp.float32)
        thin_high, thin_low = split_halves(both[:rows] + (both[rows:] + rest))
        at = slice(g * rows, (g + 1) * rows)
        left[at, :chunk] = thin_high
        left[at, chunk : 2 * chunk] = thin_low
    high, low = split_halves(col_ref[...])
    thin_high, thin_low = left[:, :chunk], left[:, chunk:]
    part = jnp.dot(thin_high, high, preferred_element_type=jnp.float32)
    part += jnp.dot(thin_low, high, preferred_element_type=jnp.float32)
    total[...] += part + jnp.dot(thin_high, low, preferred_element_type=jnp.float32)

    @pl.when(step == pl.num_programs(0) - 1)
    def _():
        shift = offset_ref[1, lax.axis_index("nest")]
        whole, part = shift // LANES, shift % LANES
        blocks = all_columns // LANES
        tiles = all_columns // STRIP
        strips = LANES // STRIP
        lane = lax.broadcasted_iota(jnp.int32, (width, LANES), 1)
        for k in range(blocks):
            turned[k] = pltpu.roll(total[:, k * LANES : (k + 1) * LANES], part, 1)

        def pack_block(i, carry):
            for k in (2 * i, 2 * i + 1):
                here = turned[lax.rem(k + blocks - whole, blocks)]
                before = turned[lax.rem(k + 2 * blocks - 1 - whole, blocks)]
                block = jnp.where(lane >= part, here, before)
                for j in range(fields // GROUP):
                    top = j * rows
                    parts = granule_transpose(
                        [block[top + f * cells : top + (f + 1) * cells] for f in range(GROUP)], STRIP
                    )
                    base = pl.multiple_of((j * tiles + k * strips) * CELLS, 8)
                    target = out_ref.at[pl.ds(base, strips * CELLS), :]
                    for t in range(strips):
                        target[t * CELLS : t * CELLS + 8, :] = parts[t]
            return carry

        lax.fori_loop(0, blocks // 2, pack_block, 0)


CHUNK = 768


def restrict(nest_offsets, row_weights, child_block, col_weights, tiles):
    fields, child_rows, child_columns = child_block.shape
    columns = col_weights.shape[1]
    cells = row_weights.shape[0]
    width = fields * cells
    rows = (fields // GROUP) * tiles * CELLS
    return pl.pallas_call(
        restrict_kernel,
        grid=(child_columns // CHUNK,),
        out_shape=jax.ShapeDtypeStruct((rows, LANES), jnp.float32),
        in_specs=[
            pl.BlockSpec(memory_space=pltpu.SMEM),
            pl.BlockSpec(row_weights.shape, lambda i: (0, 0)),
            pl.BlockSpec((fields, child_rows, CHUNK), lambda i: (0, 0, i)),
            pl.BlockSpec((CHUNK, columns), lambda i: (i, 0)),
        ],
        out_specs=pl.BlockSpec((rows, LANES), lambda i: (0, 0)),
        scratch_shapes=[
            pltpu.VMEM((GROUP * cells, 2 * LANES), jnp.float32),
            pltpu.VMEM((width, 2 * CHUNK), jnp.bfloat16),
            pltpu.VMEM((width, columns), jnp.float32),
            pltpu.VMEM((columns // LANES, width, LANES), jnp.float32),
        ],
        compiler_params=pltpu.CompilerParams(vmem_limit_bytes=60 * 2**20),
        cost_estimate=pl.CostEstimate(
            flops=6 * width * child_columns * columns,
            bytes_accessed=4 * (child_block.size + col_weights.size),
            transcendentals=0,
        ),
        name="restrict",
    )(nest_offsets.T, row_weights, child_block, col_weights)


SHARE = (GROUP + 1) * STRIP


def share_kernel(old_ref, level_ref, *outs):
    me = lax.axis_index("nest")
    nests = len(outs)
    for d in range(nests):
        first = GROUP * lax.rem(me + d, nests)
        for f in range(GROUP):
            outs[d][f * STRIP : (f + 1) * STRIP] = old_ref[first + f]
        outs[d][GROUP * STRIP :] = level_ref[...].astype(jnp.float32)


def share(parent_old, priority):
    nests = parent_old.shape[0] // GROUP
    vmem = pl.BlockSpec(memory_space=pltpu.VMEM)
    return pl.pallas_call(
        share_kernel,
        out_shape=[jax.ShapeDtypeStruct((SHARE, 2 * LANES), jnp.float32)] * nests,
        in_specs=[vmem] * 2,
        out_specs=[vmem] * nests,
        compiler_params=pltpu.CompilerParams(vmem_limit_bytes=8 * 2**20),
        name="share",
    )(parent_old, priority)


def merge_kernel(offset_ref, got_ref, *refs):
    nests = offset_ref.shape[1]
    shares = refs[:nests]
    cells, last_ref, first_ref, slab, chosen = refs[nests:]
    tiles = got_ref.shape[0] // (nests * CELLS)
    groups = tiles * CELLS // LANES
    blocks = 2 * nests
    me = lax.axis_index("nest")
    for d in range(nests):
        q = lax.rem(me + nests - d, nests)
        ref = shares[d]
        for side in range(2):
            b, at = 2 * q + side, slice(side * LANES, (side + 1) * LANES)
            for f in range(GROUP):
                cells[b, f] = ref[f * STRIP : (f + 1) * STRIP, at]
            chosen[b] = ref[GROUP * STRIP :, at]
    cells[blocks] = jnp.zeros((GROUP, STRIP, LANES), jnp.float32)
    chosen[blocks] = jnp.full((STRIP, LANES), -1.0, jnp.float32)

    def place(n, carry):
        start = offset_ref[0, n]
        whole, part = start // LANES, start % LANES
        first = pl.multiple_of(n * tiles * CELLS, 8)
        slab[pl.ds(part, tiles * CELLS), :] = got_ref[pl.ds(first, tiles * CELLS), :]
        number = n.astype(jnp.float32)
        for k in range(groups + 1):
            b = whole + k
            mine = chosen[b] == number
            upright = slab[k * LANES : (k + 1) * LANES, :].T
            for f in range(GROUP):
                value = upright[f * STRIP : (f + 1) * STRIP]
                cells[b, f] = jnp.where(mine, value, cells[b, f])
        return carry

    lax.fori_loop(0, nests, place, 0)

    def rim(b, carry):
        at = pl.ds(pl.multiple_of(b * GROUP, 8), GROUP)
        last = [cells[b, f, STRIP - 1 :, :] for f in range(GROUP)]
        last_ref[at, :] = jnp.concatenate(last, axis=0)
        first_ref[at, :] = jnp.concatenate([cells[b, f, :1, :] for f in range(GROUP)], axis=0)
        return carry

    lax.fori_loop(0, blocks, rim, 0)


def merge(offsets, got, shares):
    nests = len(shares)
    blocks = 2 * nests
    rows = got.shape[0] // nests
    vmem = pl.BlockSpec(memory_space=pltpu.VMEM)
    edge = jax.ShapeDtypeStruct((blocks * GROUP, LANES), jnp.float32)
    return pl.pallas_call(
        merge_kernel,
        out_shape=[
            jax.ShapeDtypeStruct((blocks + 1, GROUP, STRIP, LANES), jnp.float32), edge, edge
        ],
        in_specs=[pl.BlockSpec(memory_space=pltpu.SMEM)] + [vmem] * (1 + len(shares)),
        out_specs=[vmem] * 3,
        scratch_shapes=[
            pltpu.VMEM((rows + LANES, LANES), jnp.float32),
            pltpu.VMEM((blocks + 1, STRIP, LANES), jnp.float32),
        ],
        compiler_params=pltpu.CompilerParams(vmem_limit_bytes=12 * 2**20),
        name="merge",
    )(offsets.T, got, *shares)


def smooth_kernel(cells, west_ref, east_ref, rate_ref, *out_refs):
    nests = len(out_refs)
    blocks = 2 * nests
    me = lax.axis_index("nest")
    lane = lax.broadcasted_iota(jnp.int32, (STRIP, LANES), 1)
    row = lax.broadcasted_iota(jnp.int32, (STRIP, LANES), 0)

    def smooth(f, carry):
        rate = rate_ref[pl.ds(f, 1), :]
        for d in range(nests):
            q = lax.rem(me + d, nests)
            mids = [cells[2 * q, f], cells[2 * q + 1, f]]
            below = cells[jnp.maximum(2 * q - 1, 0), f]
            above = cells[jnp.minimum(2 * q + 2, blocks - 1), f]
            ups = [pltpu.roll(m, LANES - 1, 1) for m in (*mids, above)]
            downs = [pltpu.roll(m, 1, 1) for m in (below, *mids)]
            ups[2] = jnp.where(q == nests - 1, mids[1], ups[2])
            downs[0] = jnp.where(q == 0, mids[0], downs[0])
            for side in range(2):
                mid, at = mids[side], pl.ds((2 * q + side) * GROUP + f, 1)
                north = jnp.where(lane == LANES - 1, ups[side + 1], ups[side])
                south = jnp.where(lane == 0, downs[side], downs[side + 1])
                west = jnp.where(row == 0, west_ref[at, :], pltpu.roll(mid, 1, 0))
                east = jnp.where(row == STRIP - 1, east_ref[at, :], pltpu.roll(mid, STRIP - 1, 0))
                value = mid + rate * (east + west + north + south - 4.0 * mid)
                out_refs[d][f, :, side * LANES : (side + 1) * LANES] = value
        return carry

    lax.fori_loop(0, GROUP, smooth, 0)


def smooth(merged, west, east, rate):
    nests = merged.shape[0] // 2
    vmem = pl.BlockSpec(memory_space=pltpu.VMEM)
    return pl.pallas_call(
        smooth_kernel,
        out_shape=[jax.ShapeDtypeStruct((GROUP, STRIP, 2 * LANES), jnp.float32)] * nests,
        in_specs=[vmem] * 4,
        out_specs=[vmem] * nests,
        compiler_params=pltpu.CompilerParams(vmem_limit_bytes=8 * 2**20),
        name="smooth",
    )(merged, west, east, rate)


def collect_kernel(*refs):
    me = lax.axis_index("nest")
    nests = len(refs) - 1
    for d in range(nests):
        first = GROUP * lax.rem(me + nests - d, nests)
        for f in range(GROUP):
            refs[nests][first + f] = refs[d][f]


def collect(blocks):
    vmem = pl.BlockSpec(memory_space=pltpu.VMEM)
    return pl.pallas_call(
        collect_kernel,
        out_shape=jax.ShapeDtypeStruct((len(blocks) * GROUP, STRIP, 2 * LANES), jnp.float32),
        in_specs=[vmem] * len(blocks),
        out_specs=vmem,
        compiler_params=pltpu.CompilerParams(vmem_limit_bytes=4 * 2**20),
        name="collect",
    )(*blocks)


def per_device(
    child_fields, row_weights, col_weights, nest_offsets, priority, parent_old, smooth_rate
):
    tiles, nests = lax.axis_size("tile"), lax.axis_size("nest")
    nest_id = lax.axis_index("nest")
    outgoing = restrict(nest_offsets, row_weights, child_fields[0], col_weights, tiles)
    outgoing, parent_old, priority, smooth_rate = lax.optimization_barrier(
        (outgoing, parent_old, priority, smooth_rate)
    )
    got = lax.all_to_all(
        outgoing.reshape(nests * tiles, CELLS, LANES), ("nest", "tile"),
        split_axis=0, concat_axis=0, tiled=True,
    )
    got = got.reshape(nests * tiles * CELLS, LANES)

    def around(blocks):
        return [
            lax.ppermute(block, "nest", [(n, (n + d) % nests) for n in range(nests)]) if d else block
            for d, block in enumerate(blocks)
        ]

    shares = around(share(parent_old, priority))
    rate = lax.dynamic_slice_in_dim(smooth_rate, GROUP * nest_id, GROUP)
    rate = jnp.broadcast_to(rate[:, None], (GROUP, LANES))
    merged, last, first = merge(nest_offsets, got, shares)
    west = lax.ppermute(last, "tile", [(t, (t + 1) % tiles) for t in range(tiles)])
    east = lax.ppermute(first, "tile", [(t, (t - 1) % tiles) for t in range(tiles)])
    return collect(around(smooth(merged, west, east, rate)))


def solution(mesh):
    return jax.shard_map(
        per_device,
        mesh=mesh,
        in_specs=(
            P("nest", None, "tile", None),
            P(),
            P(),
            P(),
            P("tile", "nest"),
            P(None, "tile", "nest"),
            P(),
        ),
        out_specs=P(None, "tile", "nest"),
        check_vma=False,
    )
```

```python
import jax
import jax.numpy as jnp
from jax import lax
from jax.experimental import pallas as pl
from jax.experimental.pallas import tpu as pltpu
from jax.sharding import PartitionSpec as P


LANES = 128
STRIP = 16
GROUP = 8
CELLS = 8


def granule_transpose(parts, granule):
    count = len(parts)
    lane = lax.broadcasted_iota(jnp.int32, parts[0].shape, parts[0].ndim - 1)
    axis = parts[0].ndim - 1
    bit = 1
    while bit < count:
        move = bit * granule
        upper = (lane & move) != 0
        done = list(parts)
        for i in range(count):
            if not i & bit:
                a, b = parts[i], parts[i | bit]
                done[i] = jnp.where(upper, pltpu.roll(b, move, axis), a)
                done[i | bit] = jnp.where(upper, b, pltpu.roll(a, LANES - move, axis))
        parts = done
        bit *= 2
    return parts


def split_halves(value):
    high = value.astype(jnp.bfloat16)
    low = (value - high.astype(jnp.float32)).astype(jnp.bfloat16)
    return high, low


def restrict_kernel(
    offset_ref, row_ref, child_ref, col_ref, out_ref, taps, left, total, turned
):
    step = pl.program_id(0)
    fields, child_rows, chunk = child_ref.shape
    cells = row_ref.shape[0]
    width = fields * cells
    all_columns = col_ref.shape[1]
    reach = GROUP * child_rows

    @pl.when(step == 0)
    def _():
        taps[...] = jnp.zeros_like(taps)
        taps[:cells, :child_rows] = row_ref[...]
        first = taps[:cells, :]
        for f in range(1, GROUP):
            taps[f * cells : (f + 1) * cells, :] = pltpu.roll(first, f * child_rows, 1)
        total[...] = jnp.zeros_like(total)

    taps_high, taps_low = split_halves(taps[:, :reach])
    taps_both = jnp.concatenate([taps_high, taps_low], axis=0)
    rows = GROUP * cells
    for g in range(fields // GROUP):
        block = child_ref[g * GROUP : (g + 1) * GROUP].reshape(reach, chunk)
        high, low = split_halves(block)
        both = jnp.dot(taps_both, high, preferred_element_type=jnp.float32)
        rest = jnp.dot(taps_high, low, preferred_element_type=jnp.float32)
        thin_high, thin_low = split_halves(both[:rows] + (both[rows:] + rest))
        at = slice(g * rows, (g + 1) * rows)
        left[at, :chunk] = thin_high
        left[at, chunk : 2 * chunk] = thin_low
    high, low = split_halves(col_ref[...])
    thin_high, thin_low = left[:, :chunk], left[:, chunk:]
    part = jnp.dot(thin_high, high, preferred_element_type=jnp.float32)
    part += jnp.dot(thin_low, high, preferred_element_type=jnp.float32)
    total[...] += part + jnp.dot(thin_high, low, preferred_element_type=jnp.float32)

    @pl.when(step == pl.num_programs(0) - 1)
    def _():
        shift = offset_ref[1, lax.axis_index("nest")]
        whole, part = shift // LANES, shift % LANES
        blocks = all_columns // LANES
        tiles = all_columns // STRIP
        strips = LANES // STRIP
        lane = lax.broadcasted_iota(jnp.int32, (width, LANES), 1)
        for k in range(blocks):
            turned[k] = pltpu.roll(total[:, k * LANES : (k + 1) * LANES], part, 1)

        def pack_block(i, carry):
            for k in (2 * i, 2 * i + 1):
                here = turned[lax.rem(k + blocks - whole, blocks)]
                before = turned[lax.rem(k + 2 * blocks - 1 - whole, blocks)]
                block = jnp.where(lane >= part, here, before)
                for j in range(fields // GROUP):
                    top = j * rows
                    parts = granule_transpose(
                        [block[top + f * cells : top + (f + 1) * cells] for f in range(GROUP)], STRIP
                    )
                    for t in range(strips):
                        out_ref[k * strips + t, j * CELLS : (j + 1) * CELLS, :] = parts[t]
            return carry

        lax.fori_loop(0, blocks // 2, pack_block, 0)


CHUNK = 768


def restrict(nest_offsets, row_weights, child_block, col_weights, tiles):
    fields, child_rows, child_columns = child_block.shape
    columns = col_weights.shape[1]
    cells = row_weights.shape[0]
    width = fields * cells
    rows = (fields // GROUP) * CELLS
    return pl.pallas_call(
        restrict_kernel,
        grid=(child_columns // CHUNK,),
        out_shape=jax.ShapeDtypeStruct((tiles, rows, LANES), jnp.float32),
        in_specs=[
            pl.BlockSpec(memory_space=pltpu.SMEM),
            pl.BlockSpec(row_weights.shape, lambda i: (0, 0)),
            pl.BlockSpec((fields, child_rows, CHUNK), lambda i: (0, 0, i)),
            pl.BlockSpec((CHUNK, columns), lambda i: (i, 0)),
        ],
        out_specs=pl.BlockSpec((tiles, rows, LANES), lambda i: (0, 0, 0)),
        scratch_shapes=[
            pltpu.VMEM((GROUP * cells, 2 * LANES), jnp.float32),
            pltpu.VMEM((width, 2 * CHUNK), jnp.bfloat16),
            pltpu.VMEM((width, columns), jnp.float32),
            pltpu.VMEM((columns // LANES, width, LANES), jnp.float32),
        ],
        compiler_params=pltpu.CompilerParams(vmem_limit_bytes=60 * 2**20),
        cost_estimate=pl.CostEstimate(
            flops=6 * width * child_columns * columns,
            bytes_accessed=4 * (child_block.size + col_weights.size),
            transcendentals=0,
        ),
        name="restrict",
    )(nest_offsets.T, row_weights, child_block, col_weights)


SHARE = (GROUP + 1) * STRIP


def share_kernel(old_ref, level_ref, *outs):
    me = lax.axis_index("nest")
    nests = len(outs)
    for d in range(nests):
        first = GROUP * lax.rem(me + d, nests)
        for f in range(GROUP):
            outs[d][f * STRIP : (f + 1) * STRIP] = old_ref[first + f]
        outs[d][GROUP * STRIP :] = level_ref[...].astype(jnp.float32)


def share(parent_old, priority):
    nests = parent_old.shape[0] // GROUP
    vmem = pl.BlockSpec(memory_space=pltpu.VMEM)
    return pl.pallas_call(
        share_kernel,
        out_shape=[jax.ShapeDtypeStruct((SHARE, 2 * LANES), jnp.float32)] * nests,
        in_specs=[vmem] * 2,
        out_specs=[vmem] * nests,
        compiler_params=pltpu.CompilerParams(vmem_limit_bytes=8 * 2**20),
        name="share",
    )(parent_old, priority)


def merge_kernel(offset_ref, got_ref, *refs):
    nests = offset_ref.shape[1]
    shares = refs[:nests]
    cells, last_ref, first_ref, slab, chosen = refs[nests:]
    tiles = got_ref.shape[0]
    groups = tiles * CELLS // LANES
    blocks = 2 * nests
    me = lax.axis_index("nest")
    for d in range(nests):
        q = lax.rem(me + nests - d, nests)
        ref = shares[d]
        for side in range(2):
            b, at = 2 * q + side, slice(side * LANES, (side + 1) * LANES)
            for f in range(GROUP):
                cells[b, f] = ref[f * STRIP : (f + 1) * STRIP, at]
            chosen[b] = ref[GROUP * STRIP :, at]
    cells[blocks] = jnp.zeros((GROUP, STRIP, LANES), jnp.float32)
    chosen[blocks] = jnp.full((STRIP, LANES), -1.0, jnp.float32)

    def place(n, carry):
        start = offset_ref[0, n]
        whole, part = start // LANES, start % LANES
        rows = got_ref[:, pl.ds(pl.multiple_of(n * CELLS, CELLS), CELLS), :]
        slab[pl.ds(part, tiles * CELLS), :] = rows.reshape(tiles * CELLS, LANES)
        number = n.astype(jnp.float32)
        for k in range(groups + 1):
            b = whole + k
            mine = chosen[b] == number
            upright = slab[k * LANES : (k + 1) * LANES, :].T
            for f in range(GROUP):
                value = upright[f * STRIP : (f + 1) * STRIP]
                cells[b, f] = jnp.where(mine, value, cells[b, f])
        return carry

    lax.fori_loop(0, nests, place, 0)

    def rim(b, carry):
        at = pl.ds(pl.multiple_of(b * GROUP, 8), GROUP)
        last = [cells[b, f, STRIP - 1 :, :] for f in range(GROUP)]
        last_ref[at, :] = jnp.concatenate(last, axis=0)
        first_ref[at, :] = jnp.concatenate([cells[b, f, :1, :] for f in range(GROUP)], axis=0)
        return carry

    lax.fori_loop(0, blocks, rim, 0)


def merge(offsets, got, shares):
    nests = len(shares)
    blocks = 2 * nests
    rows = got.shape[0] * CELLS
    vmem = pl.BlockSpec(memory_space=pltpu.VMEM)
    edge = jax.ShapeDtypeStruct((blocks * GROUP, LANES), jnp.float32)
    return pl.pallas_call(
        merge_kernel,
        out_shape=[
            jax.ShapeDtypeStruct((blocks + 1, GROUP, STRIP, LANES), jnp.float32), edge, edge
        ],
        in_specs=[pl.BlockSpec(memory_space=pltpu.SMEM)] + [vmem] * (1 + len(shares)),
        out_specs=[vmem] * 3,
        scratch_shapes=[
            pltpu.VMEM((rows + LANES, LANES), jnp.float32),
            pltpu.VMEM((blocks + 1, STRIP, LANES), jnp.float32),
        ],
        compiler_params=pltpu.CompilerParams(vmem_limit_bytes=12 * 2**20),
        name="merge",
    )(offsets.T, got, *shares)


def smooth_kernel(cells, west_ref, east_ref, rate_ref, *out_refs):
    nests = len(out_refs)
    blocks = 2 * nests
    me = lax.axis_index("nest")
    lane = lax.broadcasted_iota(jnp.int32, (STRIP, LANES), 1)
    row = lax.broadcasted_iota(jnp.int32, (STRIP, LANES), 0)

    def smooth(f, carry):
        rate = rate_ref[pl.ds(f, 1), :]
        for d in range(nests):
            q = lax.rem(me + d, nests)
            mids = [cells[2 * q, f], cells[2 * q + 1, f]]
            below = cells[jnp.maximum(2 * q - 1, 0), f]
            above = cells[jnp.minimum(2 * q + 2, blocks - 1), f]
            ups = [pltpu.roll(m, LANES - 1, 1) for m in (*mids, above)]
            downs = [pltpu.roll(m, 1, 1) for m in (below, *mids)]
            ups[2] = jnp.where(q == nests - 1, mids[1], ups[2])
            downs[0] = jnp.where(q == 0, mids[0], downs[0])
            for side in range(2):
                mid, at = mids[side], pl.ds((2 * q + side) * GROUP + f, 1)
                north = jnp.where(lane == LANES - 1, ups[side + 1], ups[side])
                south = jnp.where(lane == 0, downs[side], downs[side + 1])
                west = jnp.where(row == 0, west_ref[at, :], pltpu.roll(mid, 1, 0))
                east = jnp.where(row == STRIP - 1, east_ref[at, :], pltpu.roll(mid, STRIP - 1, 0))
                value = mid + rate * (east + west + north + south - 4.0 * mid)
                out_refs[d][f, :, side * LANES : (side + 1) * LANES] = value
        return carry

    lax.fori_loop(0, GROUP, smooth, 0)


def smooth(merged, west, east, rate):
    nests = merged.shape[0] // 2
    vmem = pl.BlockSpec(memory_space=pltpu.VMEM)
    return pl.pallas_call(
        smooth_kernel,
        out_shape=[jax.ShapeDtypeStruct((GROUP, STRIP, 2 * LANES), jnp.float32)] * nests,
        in_specs=[vmem] * 4,
        out_specs=[vmem] * nests,
        compiler_params=pltpu.CompilerParams(vmem_limit_bytes=8 * 2**20),
        name="smooth",
    )(merged, west, east, rate)


def collect_kernel(*refs):
    me = lax.axis_index("nest")
    nests = len(refs) - 1
    for d in range(nests):
        first = GROUP * lax.rem(me + nests - d, nests)
        for f in range(GROUP):
            refs[nests][first + f] = refs[d][f]


def collect(blocks):
    vmem = pl.BlockSpec(memory_space=pltpu.VMEM)
    return pl.pallas_call(
        collect_kernel,
        out_shape=jax.ShapeDtypeStruct((len(blocks) * GROUP, STRIP, 2 * LANES), jnp.float32),
        in_specs=[vmem] * len(blocks),
        out_specs=vmem,
        compiler_params=pltpu.CompilerParams(vmem_limit_bytes=4 * 2**20),
        name="collect",
    )(*blocks)


def per_device(
    child_fields, row_weights, col_weights, nest_offsets, priority, parent_old, smooth_rate
):
    tiles, nests = lax.axis_size("tile"), lax.axis_size("nest")
    nest_id = lax.axis_index("nest")
    outgoing = restrict(nest_offsets, row_weights, child_fields[0], col_weights, tiles)
    outgoing, parent_old, priority, smooth_rate = lax.optimization_barrier(
        (outgoing, parent_old, priority, smooth_rate)
    )
    got = lax.all_to_all(
        outgoing.reshape(tiles * nests, CELLS, LANES), ("tile", "nest"),
        split_axis=0, concat_axis=0, tiled=True,
    )
    got = got.reshape(tiles, nests * CELLS, LANES)

    def around(blocks):
        return [
            lax.ppermute(block, "nest", [(n, (n + d) % nests) for n in range(nests)]) if d else block
            for d, block in enumerate(blocks)
        ]

    shares = around(share(parent_old, priority))
    rate = lax.dynamic_slice_in_dim(smooth_rate, GROUP * nest_id, GROUP)
    rate = jnp.broadcast_to(rate[:, None], (GROUP, LANES))
    merged, last, first = merge(nest_offsets, got, shares)
    west = lax.ppermute(last, "tile", [(t, (t + 1) % tiles) for t in range(tiles)])
    east = lax.ppermute(first, "tile", [(t, (t - 1) % tiles) for t in range(tiles)])
    return collect(around(smooth(merged, west, east, rate)))


def solution(mesh):
    return jax.shard_map(
        per_device,
        mesh=mesh,
        in_specs=(
            P("nest", None, "tile", None),
            P(),
            P(),
            P(),
            P("tile", "nest"),
            P(None, "tile", "nest"),
            P(),
        ),
        out_specs=P(None, "tile", "nest"),
        check_vma=False,
    )
```
